32 devices in a mesh: job: 2 (over core), replica: 4 (over z), model: 4 (over y, x).
Axes of the slice: x: 2, y: 2, z: 4, core: 2. Of those that a mesh axis runs over, the one named last changes fastest.
Arguments:
- grad_query: float32 [8, 1024, 1024], P(('job', 'replica'), None, 'model'), parts along dimension 0, may hold values from -0.875 to 0.875
- grad_key: float32 [8, 1024, 1024], P(('job', 'replica'), None, 'model'), parts along dimension 0, may hold values from -0.875 to 0.875
- grad_value: float32 [8, 1024, 1024], P(('job', 'replica'), None, 'model'), parts along dimension 0, may hold values from -0.875 to 0.875
- grad_mixed: float32 [8, 1024, 1024], P(('job', 'replica'), 'model'), parts along dimension 0, may hold values from -0.875 to 0.875
- grad_norm: float32 [8, 1024], P(('job', 'replica')), parts along dimension 0, may hold values from -8 to 8
- weight_query: float32 [2048, 1024], P(('job', 'replica'), 'model'), parts along dimension 0, may hold values from -0.25 to 0.25
- weight_key: float32 [2048, 1024], P(('job', 'replica'), 'model'), parts along dimension 0, may hold values from -0.25 to 0.25
- weight_value: float32 [2048, 1024], P(('job', 'replica'), 'model'), parts along dimension 0, may hold values from -0.25 to 0.25
- weight_mixed: float32 [2048, 1024], P(('job', 'model'), 'replica'), parts along dimension 0, may hold values from -0.25 to 0.25
- weight_norm: float32 [2048], P(('job', 'replica')), parts along dimension 0, may hold values from 0.25 to 1.75
- moment_query: float32 [2048, 1024], P(('job', 'replica'), 'model'), parts along dimension 0, may hold values from -0.1875 to 0.1875
- moment_key: float32 [2048, 1024], P(('job', 'replica'), 'model'), parts along dimension 0, may hold values from -0.1875 to 0.1875
- moment_value: float32 [2048, 1024], P(('job', 'replica'), 'model'), parts along dimension 0, may hold values from -0.1875 to 0.1875
- moment_mixed: float32 [2048, 1024], P(('job', 'model'), 'replica'), parts along dimension 0, may hold values from -0.1875 to 0.1875
- moment_norm: float32 [2048], P(('job', 'replica')), parts along dimension 0, may hold values from -1.75 to 1.75
Outputs:
- copy_query: bfloat16 [2048, 1024], P('job', 'model'), parts along dimension 0
- copy_key: bfloat16 [2048, 1024], P('job', 'model'), parts along dimension 0
- copy_value: bfloat16 [2048, 1024], P('job', 'model'), parts along dimension 0
- copy_mixed: bfloat16 [2048, 1024], P(('job', 'model')), parts along dimension 0
- copy_norm: bfloat16 [2048], P('job'), parts along dimension 0
- new_query: float32 [2048, 1024], P(('job', 'replica'), 'model'), parts along dimension 0
- new_key: float32 [2048, 1024], P(('job', 'replica'), 'model'), parts along dimension 0
- new_value: float32 [2048, 1024], P(('job', 'replica'), 'model'), parts along dimension 0
- new_mixed: float32 [2048, 1024], P(('job', 'model'), 'replica'), parts along dimension 0
- new_norm: float32 [2048], P(('job', 'replica')), parts along dimension 0
- state_new_query: float32 [2048, 1024], P(('job', 'replica'), 'model'), parts along dimension 0
- state_new_key: float32 [2048, 1024], P(('job', 'replica'), 'model'), parts along dimension 0
- state_new_value: float32 [2048, 1024], P(('job', 'replica'), 'model'), parts along dimension 0
- state_new_mixed: float32 [2048, 1024], P(('job', 'model'), 'replica'), parts along dimension 0
- state_new_norm: float32 [2048], P(('job', 'replica')), parts along dimension 0
The draws below stay inside these ranges and needn't reach their ends.
There are 2 independent parts, one for each index of `job`. The reference program is written for one: setup_inputs(seed, part) draws one part's arguments, and reference() takes and returns one part's arrays. A program takes and returns all parts, laid end to end along the dimension named above; each array names one. Nothing has to cross between parts.
All inputs are finite; a program needn't handle non-finite values.
Results may differ from the reference program's by a relative error of at most 0.0004.
Values may be sent and summed in bfloat16 or wider, within the bound.
No kernel may reach another device: no remote copies, remote signals or barrier semaphores. Data moves between devices by JAX's collectives and lax.ppermute only.
A program may use at most 64 MiB of HBM per device.

```python
import jax
import jax.numpy as jnp
from jax import lax

WIDTH = 1024
ATTN = 1024
REPLICAS = 4


def with_spikes(result, stream_key, source, target, blocks, factor):
    def block_of(axis_at):
        return (jnp.arange(result.shape[axis_at]) // (result.shape[axis_at] // blocks)).reshape((-1,) + (1,) * (result.ndim - 1 - axis_at))

    near = jax.random.permutation(stream_key, blocks)[block_of(target)]
    other_side = (block_of(target) + blocks // 2) % blocks
    return jnp.where((block_of(source) == near) | (block_of(source) == other_side), factor * result, result)


def levels(rng, extent, shards, low, largest):
    loudness, own = 1.0, jax.random.fold_in(rng, 6)
    for axis_at, shards_of in shards:
        steps = jnp.exp(jax.random.uniform(jax.random.fold_in(own, axis_at), (shards_of,), jnp.float32, low / len(shards), largest / len(shards)))
        loudness = loudness * jnp.repeat(steps, extent[axis_at] // shards_of).reshape([-1 if axis == axis_at else 1 for axis in range(len(extent))])
    return loudness


def noise(rng, dims, width, bound, pieces=(), dtype=jnp.bfloat16):
    entries = jax.random.normal(rng, dims, jnp.float32) * width
    if len(pieces) > 0:
        entries = levels(rng, dims, pieces, -0.22, 0.18) * entries
    return jnp.clip(entries, min=-bound, max=bound).astype(dtype)


def heavy_noise(stream_key, dims, width, most, pieces, heavy, dtype=jnp.bfloat16):
    result = width * jax.random.normal(stream_key, dims, jnp.float32)
    if pieces:
        result = result * levels(stream_key, dims, pieces, -0.22, 0.18)
    return jnp.clip(with_spikes(result, jax.random.fold_in(stream_key, 3), *heavy), -most, most).astype(dtype)


def setup_inputs(seed: int = 0, part: int = 0) -> dict:
    streams_of = jax.random.split(jax.random.key(seed), 16)
    part_splits = jax.random.split(jax.random.fold_in(streams_of[15], part), 16)
    return {
        "grad_query": heavy_noise(part_splits[0], (REPLICAS, WIDTH, ATTN), 0.1, 0.875, ((0, 4), (2, 4)), (0, 1, 4, 2.0), jnp.float32),
        "grad_key": heavy_noise(part_splits[1], (REPLICAS, WIDTH, ATTN), 0.1, 0.875, ((0, 4), (2, 4)), (0, 1, 4, 2.0), jnp.float32),
        "grad_value": heavy_noise(part_splits[2], (REPLICAS, WIDTH, ATTN), 0.1, 0.875, ((0, 4), (2, 4)), (0, 1, 4, 2.0), jnp.float32),
        "grad_mixed": heavy_noise(part_splits[3], (REPLICAS, ATTN, WIDTH), 0.1, 0.875, ((0, 4), (1, 4)), (0, 2, 4, 2.0), jnp.float32),
        "grad_norm": heavy_noise(part_splits[4], (REPLICAS, WIDTH), 1.0, 8.0, ((0, 4),), (0, 1, 4, 2.0), jnp.float32),
        "weight_query": heavy_noise(part_splits[5], (WIDTH, ATTN), WIDTH ** -0.5, 0.25, ((0, 4), (1, 4)), (1, 0, 4, 2.0), jnp.float32),
        "weight_key": heavy_noise(part_splits[6], (WIDTH, ATTN), WIDTH ** -0.5, 0.25, ((0, 4), (1, 4)), (1, 0, 4, 2.0), jnp.float32),
        "weight_value": heavy_noise(part_splits[7], (WIDTH, ATTN), WIDTH ** -0.5, 0.25, ((0, 4), (1, 4)), (1, 0, 4, 2.0), jnp.float32),
        "weight_mixed": heavy_noise(part_splits[8], (ATTN, WIDTH), ATTN ** -0.5, 0.25, ((0, 4), (1, 4)), (0, 1, 4, 2.0), jnp.float32),
        "weight_norm": jnp.clip(1.0 + 0.15 * jax.random.normal(part_splits[9], (WIDTH,), jnp.float32), 0.25, 1.75),
        "moment_query": noise(part_splits[10], (WIDTH, ATTN), WIDTH ** -0.5, 0.1875, ((0, 4), (1, 4)), jnp.float32),
        "moment_key": noise(part_splits[11], (WIDTH, ATTN), WIDTH ** -0.5, 0.1875, ((0, 4), (1, 4)), jnp.float32),
        "moment_value": noise(part_splits[12], (WIDTH, ATTN), WIDTH ** -0.5, 0.1875, ((0, 4), (1, 4)), jnp.float32),
        "moment_mixed": noise(part_splits[13], (ATTN, WIDTH), ATTN ** -0.5, 0.1875, ((0, 4), (1, 4)), jnp.float32),
        "moment_norm": noise(part_splits[14], (WIDTH,), 0.3, 1.75, ((0, 4),), jnp.float32),
    }


learn_rate = 0.5
hold_rate = 0.9

def reference(grad_query, grad_key, grad_value, grad_mixed, grad_norm, weight_query, weight_key, weight_value, weight_mixed, weight_norm, moment_query, moment_key, moment_value, moment_mixed, moment_norm):
    mean_query = lax.optimization_barrier(jnp.sum(grad_query.astype(jnp.float32), axis=0)) * REPLICAS ** (-0.5)
    mean_key = lax.optimization_barrier(jnp.sum(grad_key.astype(jnp.float32), axis=0)) * REPLICAS ** (-0.5)
    mean_value = lax.optimization_barrier(jnp.sum(grad_value.astype(jnp.float32), axis=0)) * REPLICAS ** (-0.5)
    mean_mixed = lax.optimization_barrier(jnp.sum(grad_mixed.astype(jnp.float32), axis=0)) * REPLICAS ** (-0.5)
    mean_norm = lax.optimization_barrier(jnp.sum(grad_norm.astype(jnp.float32), axis=0)) * REPLICAS ** (-0.5)
    ratio_query = jnp.sqrt(lax.optimization_barrier(jnp.sum(weight_query * weight_query, axis=1, keepdims=True))) * lax.rsqrt(lax.optimization_barrier(jnp.sum(mean_query * mean_query, axis=1, keepdims=True)) + 1e-06)
    mean_query = mean_query * ratio_query
    ratio_key = jnp.sqrt(lax.optimization_barrier(jnp.sum(weight_key * weight_key, axis=1, keepdims=True))) * lax.rsqrt(lax.optimization_barrier(jnp.sum(mean_key * mean_key, axis=1, keepdims=True)) + 1e-06)
    mean_key = mean_key * ratio_key
    ratio_value = jnp.sqrt(lax.optimization_barrier(jnp.sum(weight_value * weight_value, axis=1, keepdims=True))) * lax.rsqrt(lax.optimization_barrier(jnp.sum(mean_value * mean_value, axis=1, keepdims=True)) + 1e-06)
    mean_value = mean_value * ratio_value
    ratio_mixed = jnp.sqrt(lax.optimization_barrier(jnp.sum(weight_mixed * weight_mixed, axis=0, keepdims=True))) * lax.rsqrt(lax.optimization_barrier(jnp.sum(mean_mixed * mean_mixed, axis=0, keepdims=True)) + 1e-06)
    mean_mixed = mean_mixed * ratio_mixed
    state_new_query = hold_rate * moment_query + mean_query
    new_query = weight_query - learn_rate * state_new_query
    state_new_key = hold_rate * moment_key + mean_key
    new_key = weight_key - learn_rate * state_new_key
    state_new_value = hold_rate * moment_value + mean_value
    new_value = weight_value - learn_rate * state_new_value
    state_new_mixed = hold_rate * moment_mixed + mean_mixed
    new_mixed = weight_mixed - learn_rate * state_new_mixed
    state_new_norm = hold_rate * moment_norm + mean_norm
    new_norm = weight_norm - learn_rate * state_new_norm
    copy_query = new_query.astype(jnp.bfloat16)
    copy_key = new_key.astype(jnp.bfloat16)
    copy_value = new_value.astype(jnp.bfloat16)
    copy_mixed = new_mixed.astype(jnp.bfloat16)
    copy_norm = new_norm.astype(jnp.bfloat16)
    return (copy_query, copy_key, copy_value, copy_mixed, copy_norm, new_query, new_key, new_value, new_mixed, new_norm, state_new_query, state_new_key, state_new_value, state_new_mixed, state_new_norm)
```

```python
import jax
import jax.numpy as jnp
from jax import lax
from jax.experimental import pallas as pl
from jax.experimental.pallas import tpu as pltpu
from jax.sharding import PartitionSpec as P

learn_rate = 0.5
hold_rate = 0.9
WIRE = jnp.float16
F32 = jnp.float32
PAD = 8
LEVELS = 30.0 * 1024.0 - 1.0
LEAST = 2.0**-28
ROW_SCALE = 2.0**14
NORM_SCALE = 2.0**10


def general(
    grad_query,
    grad_key,
    grad_value,
    grad_mixed,
    grad_norm,
    weight_query,
    weight_key,
    weight_value,
    weight_mixed,
    weight_norm,
    moment_query,
    moment_key,
    moment_value,
    moment_mixed,
    moment_norm,
):
    rate = lax.axis_size("replica") ** (-0.5)
    grads = (grad_query, grad_key, grad_value, grad_mixed)
    weights = (weight_query, weight_key, weight_value, weight_mixed)
    moments = (moment_query, moment_key, moment_value, moment_mixed)
    cuts = (0, 0, 0, 1)
    means = [
        lax.psum_scatter(g[0], "replica", scatter_dimension=c, tiled=True) * rate
        for g, c in zip(grads, cuts)
    ]
    whole = lax.psum(grad_norm[0], "replica")
    place = lax.axis_index("replica")
    size = weight_norm.shape[0]
    mean_norm = lax.dynamic_slice_in_dim(whole, place * size, size) * rate
    sums = lax.psum(
        tuple(jnp.sum(w * w, axis=1 - c, keepdims=True) for w, c in zip(weights, cuts))
        + tuple(jnp.sum(m * m, axis=1 - c, keepdims=True) for m, c in zip(means, cuts)),
        "model",
    )
    states, news = [], []
    for i in range(4):
        mean = means[i] * (jnp.sqrt(sums[i]) * lax.rsqrt(sums[4 + i] + 1e-06))
        states.append(hold_rate * moments[i] + mean)
        news.append(weights[i] - learn_rate * states[i])
    states.append(hold_rate * moment_norm + mean_norm)
    news.append(weight_norm - learn_rate * states[4])
    copies = [
        lax.all_gather(new.astype(jnp.bfloat16), "replica", axis=c, tiled=True)
        for new, c in zip(news, (0, 0, 0, 1, 0))
    ]
    return (*copies, *news, *states)


def cost(bytes_):
    return pl.CostEstimate(flops=bytes_, bytes_accessed=bytes_, transcendentals=0)


def vmem():
    return pl.BlockSpec(memory_space=pltpu.VMEM)


def anywhere():
    return pl.BlockSpec(memory_space=pl.ANY)


def as_row(column):
    return column.T[0:1, :]


def as_column(row, side):
    lanes = jnp.broadcast_to(row, (128, side)).T
    return jnp.concatenate([lanes] * (side // 128), axis=1)


def code(x, by_column):
    side = x.shape[0]
    size = jnp.abs(x)
    if by_column:
        top = jnp.max(size, axis=0, keepdims=True)
        row = jnp.maximum((top * 1.01).astype(jnp.bfloat16).astype(F32), LEAST)
        scale = row
    else:
        top = jnp.broadcast_to(jnp.max(size, axis=1, keepdims=True), (side, 128))
        lanes = jnp.maximum((top * 1.01).astype(jnp.bfloat16).astype(F32), LEAST)
        row = as_row(lanes)
        scale = jnp.concatenate([lanes] * (side // 128), axis=1)
    level = jnp.round(size * (LEVELS / scale))
    power = jnp.floor(level * (1.0 / 1024.0))
    number = (level + (1024.0 - 1024.0 * power)) * jnp.exp2(power - 24.0)
    return jnp.where(x < 0, -number, number), row


def decode(number, row, by_column):
    side = number.shape[0]
    size = jnp.abs(number)
    power = jnp.floor(jnp.log2(size * (1.0 + 2.0**-12)) + 14.0)
    level = 1024.0 * (power + size * jnp.exp2(14.0 - power) - 1.0)
    unit = row * (1.0 / LEVELS)
    unit = unit if by_column else as_column(unit, side)
    return jnp.where(number < 0, -level, level) * unit


def write_message(out, blocks, norm, columns, side):
    k = len(blocks)
    rows = []
    for j in range(k):
        number, row = code(blocks[j], columns[j])
        out[j * side : (j + 1) * side, :] = number
        rows.append(row * ROW_SCALE)
    if norm is not None:
        norm = norm * NORM_SCALE
        high = norm.astype(jnp.bfloat16).astype(F32)
        rows += [high, norm - high]
    for j in range(PAD):
        out[k * side + j : k * side + j + 1, :] = rows[min(j, len(rows) - 1)]


def read_message(got, columns, with_norm, side):
    k = len(columns)
    row = lambda j: got[k * side + j : k * side + j + 1, :]
    blocks = [
        decode(got[j * side : (j + 1) * side, :], row(j) * (1.0 / ROW_SCALE), columns[j])
        for j in range(k)
    ]
    norm = (row(k) + row(k + 1)) * (1.0 / NORM_SCALE) if with_norm else None
    return blocks, norm


def fetch(grad_refs, held, sem, columns, slot, side):
    start = pl.multiple_of((lax.axis_index("replica") ^ slot) * side, side)
    moves = []
    for j, ref in enumerate(grad_refs):
        part = ref.at[0, :, pl.ds(start, side)] if columns[j] else ref.at[0, pl.ds(start, side), :]
        moves.append(pltpu.make_async_copy(part, held.at[j], sem.at[j]))
    for move in moves:
        move.start()
    return moves


def norm_row(norm_ref, slot, side):
    start = pl.multiple_of((lax.axis_index("replica") ^ slot) * side, side)
    return norm_ref[0:1, pl.ds(start, side)]


def send_block(grads, columns, norm, got, side, slot, name):
    k = len(grads)
    rows = k * side + PAD

    def body(*refs):
        refs = list(refs)
        grad_refs = [refs.pop(0) for _ in range(k)]
        norm_ref = refs.pop(0) if norm is not None else None
        got_ref = refs.pop(0) if got is not None else None
        out, held, sem = refs
        moves = fetch(grad_refs, held, sem, columns, slot, side)
        row = norm_row(norm_ref, slot, side) if norm is not None else None
        more = [None] * k
        if got is not None:
            more, more_norm = read_message(got_ref, columns, norm is not None, side)
            row = row + more_norm if norm is not None else None
        for move in moves:
            move.wait()
        blocks = [held[j] if more[j] is None else held[j] + more[j] for j in range(k)]
        write_message(out, blocks, row, columns, side)

    specs, args = [anywhere()] * k, list(grads)
    if norm is not None:
        specs.append(vmem())
        args.append(norm)
    if got is not None:
        specs.append(vmem())
        args.append(got)
    return pl.pallas_call(
        body,
        out_shape=jax.ShapeDtypeStruct((rows, side), F32),
        in_specs=specs,
        out_specs=vmem(),
        scratch_shapes=[pltpu.VMEM((k, side, side), F32), pltpu.SemaphoreType.DMA((k,))],
        cost_estimate=cost(k * side * side * 16),
        name=name,
    )(*args)


def slice_sums(square, by_column):
    if by_column:
        return jnp.sum(square, axis=0, keepdims=True)
    side = square.shape[0]
    lanes = square[:, :128]
    for start in range(128, side, 128):
        lanes = lanes + square[:, start : start + 128]
    return jnp.sum(lanes.T, axis=0, keepdims=True)


def means(grads, columns, norm, weights, gots, side, rate, name):
    k = len(grads)

    def body(*refs):
        refs = list(refs)
        grad_refs = [refs.pop(0) for _ in range(k)]
        norm_ref = refs.pop(0) if norm is not None else None
        weight_refs = [refs.pop(0) for _ in range(k)]
        got_refs = [refs.pop(0) for _ in gots]
        mean_ref, sum_ref, held, sem = refs
        moves = fetch(grad_refs, held, sem, columns, 0, side)
        row = norm_row(norm_ref, 0, side) if norm is not None else None
        totals = [None] * k
        for got_ref in got_refs:
            blocks, more = read_message(got_ref, columns, norm is not None, side)
            totals = [b if t is None else t + b for t, b in zip(totals, blocks)]
            row = row + more if norm is not None else None
        for move in moves:
            move.wait()
        for j in range(k):
            mean = (held[j] + totals[j]) * rate
            mean_ref[j * side : (j + 1) * side, :] = mean
            weight = weight_refs[j][...]
            sum_ref[2 * j : 2 * j + 1, :] = slice_sums(weight * weight, columns[j])
            sum_ref[2 * j + 1 : 2 * j + 2, :] = slice_sums(mean * mean, columns[j])
        if norm is not None:
            mean_ref[k * side :, :] = jnp.broadcast_to(row * rate, (PAD, side))

    specs, args = [anywhere()] * k, list(grads)
    if norm is not None:
        specs.append(vmem())
        args.append(norm)
    args += [*weights, *gots]
    specs += [vmem()] * (k + len(gots))
    rows = k * side + (PAD if norm is not None else 0)
    return pl.pallas_call(
        body,
        out_shape=[
            jax.ShapeDtypeStruct((rows, side), F32),
            jax.ShapeDtypeStruct((2 * k, side), F32),
        ],
        in_specs=specs,
        out_specs=[vmem()] * 2,
        scratch_shapes=[pltpu.VMEM((k, side, side), F32), pltpu.SemaphoreType.DMA((k,))],
        cost_estimate=cost(k * side * side * 24),
        name=name,
    )(*args)


def update(mean, sums, weights, moments, columns, norm, side, name):
    k = len(weights)

    def body(*refs):
        refs = list(refs)
        mean_ref = refs.pop(0)
        sum_refs = [refs.pop(0) for _ in sums]
        weight_refs = [refs.pop(0) for _ in range(k)]
        moment_refs = [refs.pop(0) for _ in range(k)]
        norm_refs = [refs.pop(0) for _ in range(2)] if norm is not None else None
        send_ref = refs.pop(0)
        new_refs = [refs.pop(0) for _ in range(k)]
        state_refs = [refs.pop(0) for _ in range(k)]
        total = sum_refs[0][...]
        for s in sum_refs[1:]:
            total = total + s[...]
        for j in range(k):
            part = slice(j * side, (j + 1) * side)
            ratio = jnp.sqrt(total[2 * j : 2 * j + 1, :]) * lax.rsqrt(
                total[2 * j + 1 : 2 * j + 2, :] + 1e-06
            )
            full = ratio if columns[j] else as_column(ratio, side)
            state = hold_rate * moment_refs[j][...] + mean_ref[part, :] * full
            new = weight_refs[j][...] - learn_rate * state
            state_refs[j][...] = state
            new_refs[j][...] = new
            send_ref[part, :] = new.astype(jnp.bfloat16)
        if norm is not None:
            new_ref, state_ref = refs.pop(0), refs.pop(0)
            row = mean_ref[k * side : k * side + 1, :]
            state = hold_rate * norm_refs[1][...] + row
            new = norm_refs[0][...] - learn_rate * state
            state_ref[...] = state
            new_ref[...] = new
            send_ref[k * side :, :] = jnp.broadcast_to(new, (PAD, side)).astype(jnp.bfloat16)

    args = [mean, *sums, *weights, *moments]
    square = jax.ShapeDtypeStruct((side, side), F32)
    outs = [jax.ShapeDtypeStruct(mean.shape, jnp.bfloat16)] + [square] * (2 * k)
    if norm is not None:
        args += list(norm)
        outs += [jax.ShapeDtypeStruct((1, side), F32)] * 2
    return pl.pallas_call(
        body,
        out_shape=outs,
        in_specs=[vmem() for _ in args],
        out_specs=[vmem() for _ in outs],
        cost_estimate=cost(k * side * side * 22),
        name=name,
    )(*args)


def assemble(blocks, columns, with_norm, side, name):
    k, n = len(columns), len(blocks)

    def body(*refs):
        ins, outs, sem = refs[:n], refs[n:-1], refs[-1]
        starts = [
            pl.multiple_of((lax.axis_index("replica") ^ slot) * side, side) for slot in range(n)
        ]
        moves = []
        for slot in range(n):
            for j in range(k):
                part = ins[slot].at[j * side : (j + 1) * side, :]
                if columns[j]:
                    to = outs[j].at[:, pl.ds(starts[slot], side)]
                else:
                    to = outs[j].at[pl.ds(starts[slot], side), :]
                moves.append(pltpu.make_async_copy(part, to, sem.at[slot * k + j]))
        for move in moves:
            move.start()
        if with_norm:
            for slot in range(n):
                row = ins[slot][k * side : k * side + 1, :]
                outs[k][0:1, pl.ds(starts[slot], side)] = row
        for move in moves:
            move.wait()

    outs, specs = [], []
    for c in columns:
        shape = (side, n * side) if c else (n * side, side)
        outs.append(jax.ShapeDtypeStruct(shape, jnp.bfloat16))
        specs.append(anywhere())
    if with_norm:
        outs.append(jax.ShapeDtypeStruct((1, n * side), jnp.bfloat16))
        specs.append(vmem())
    return pl.pallas_call(
        body,
        out_shape=outs,
        in_specs=[vmem()] * n,
        out_specs=specs,
        scratch_shapes=[pltpu.SemaphoreType.DMA((n * k,))],
        cost_estimate=cost(n * k * side * side * 4),
        name=name,
    )(*blocks)


def four(
    grad_query,
    grad_key,
    grad_value,
    grad_mixed,
    grad_norm,
    weight_query,
    weight_key,
    weight_value,
    weight_mixed,
    weight_norm,
    moment_query,
    moment_key,
    moment_value,
    moment_mixed,
    moment_norm,
):
    n, m = lax.axis_size("replica"), lax.axis_size("model")
    side = weight_query.shape[0]
    rate = n ** (-0.5)

    def swap(x, bit, name, axis="replica"):
        with jax.named_scope(name):
            return lax.ppermute(x, axis, [(i, i ^ bit) for i in range(lax.axis_size(axis))])

    def carry(x, bit, name):
        return swap(x.astype(WIRE), bit, name).astype(F32)

    grads = (grad_query, grad_key, grad_value, grad_mixed)
    weights = (weight_query, weight_key, weight_value, weight_mixed)
    moments = (moment_query, moment_key, moment_value, moment_mixed)
    columns = (False, False, False, True)
    norm_values = (weight_norm.reshape(1, side), moment_norm.reshape(1, side))
    copies, news, states = {}, {}, {}
    for tag, group, has_norm in (("a", (0, 1), True), ("b", (2, 3), False)):
        pick = lambda xs: [xs[j] for j in group]
        cols, own_grads = pick(columns), pick(grads)
        norm = grad_norm if has_norm else None
        block = lambda slot, got, name: send_block(
            own_grads, cols, norm, got, side, slot, name + tag
        )
        if tag == "a":
            gots = [
                carry(block(slot, None, f"block{slot}"), slot, f"send{slot}{tag}")
                for slot in (3, 2, 1)
            ]
        else:
            far = carry(block(3, None, "far"), 1, "send3" + tag)
            near = carry(block(1, None, "near"), 1, "send1" + tag)
            gots = [near, carry(block(2, far, "half"), 2, "send2" + tag)]
        mean, sums = means(
            own_grads, cols, norm, pick(weights), gots, side, rate, "means" + tag
        )
        parts = [sums] + [swap(sums, bit, f"sums{bit}{tag}", "model") for bit in range(1, m)]
        out = update(
            mean, parts, pick(weights), pick(moments), cols,
            norm_values if has_norm else None, side, "update" + tag,
        )
        own = out[0]
        two = swap(own, 2, "copy2" + tag)
        one = swap(own, 1, "copy1" + tag)
        three = swap(two, 1, "copy3" + tag) if tag == "a" else swap(own, 3, "copy3" + tag)
        whole = assemble([own, one, two, three], cols, has_norm, side, "assemble" + tag)
        k = len(group)
        for i, j in enumerate(group):
            copies[j], news[j], states[j] = whole[i], out[1 + i], out[1 + k + i]
        if has_norm:
            copies[4] = whole[k].reshape(-1)
            news[4], states[4] = out[1 + 2 * k].reshape(-1), out[2 + 2 * k].reshape(-1)
    return tuple(d[j] for d in (copies, news, states) for j in range(5))


def local(*args):
    n, m = lax.axis_size("replica"), lax.axis_size("model")
    rows, cols = args[5].shape
    square = all(a.shape == (rows, rows) for a in args[5:9]) and rows % 128 == 0
    if n == 4 and m & (m - 1) == 0 and square and args[9].shape == (rows,):
        return four(*args)
    return general(*args)


def solution(mesh):
    lead, wide = ("job", "replica"), ("job", "model")
    grads = (P(lead, None, "model"),) * 3 + (P(lead, "model", None), P(lead, None))
    shards = (P(lead, "model"),) * 3 + (P(wide, "replica"), P(lead))
    copies = (P("job", "model"),) * 3 + (P(wide, None), P("job"))
    return jax.shard_map(
        local,
        mesh=mesh,
        in_specs=grads + shards + shards,
        out_specs=copies + shards + shards,
        check_vma=False,
    )
```

```python
import jax
import jax.numpy as jnp
from jax import lax
from jax.experimental import pallas as pl
from jax.experimental.pallas import tpu as pltpu
from jax.sharding import PartitionSpec as P


learn_rate = 0.5
hold_rate = 0.9
WIRE = jnp.float16
F32 = jnp.float32
PAD = 8
LEVELS = 30.0 * 1024.0 - 1.0
LEAST = 2.0**-28
ROW_SCALE = 2.0**14
NORM_SCALE = 2.0**10
GRANT = 10 * 2**20


def general(
    grad_query,
    grad_key,
    grad_value,
    grad_mixed,
    grad_norm,
    weight_query,
    weight_key,
    weight_value,
    weight_mixed,
    weight_norm,
    moment_query,
    moment_key,
    moment_value,
    moment_mixed,
    moment_norm,
):
    rate = lax.axis_size("replica") ** (-0.5)
    grads = (grad_query, grad_key, grad_value, grad_mixed)
    weights = (weight_query, weight_key, weight_value, weight_mixed)
    moments = (moment_query, moment_key, moment_value, moment_mixed)
    cuts = (0, 0, 0, 1)
    means = [
        lax.psum_scatter(g[0], "replica", scatter_dimension=c, tiled=True) * rate
        for g, c in zip(grads, cuts)
    ]
    whole = lax.psum(grad_norm[0], "replica")
    place = lax.axis_index("replica")
    size = weight_norm.shape[0]
    mean_norm = lax.dynamic_slice_in_dim(whole, place * size, size) * rate
    sums = lax.psum(
        tuple(jnp.sum(w * w, axis=1 - c, keepdims=True) for w, c in zip(weights, cuts))
        + tuple(jnp.sum(m * m, axis=1 - c, keepdims=True) for m, c in zip(means, cuts)),
        "model",
    )
    states, news = [], []
    for i in range(4):
        mean = means[i] * (jnp.sqrt(sums[i]) * lax.rsqrt(sums[4 + i] + 1e-06))
        states.append(hold_rate * moments[i] + mean)
        news.append(weights[i] - learn_rate * states[i])
    states.append(hold_rate * moment_norm + mean_norm)
    news.append(weight_norm - learn_rate * states[4])
    copies = [
        lax.all_gather(new.astype(jnp.bfloat16), "replica", axis=c, tiled=True)
        for new, c in zip(news, (0, 0, 0, 1, 0))
    ]
    return (*copies, *news, *states)


def cost(bytes_):
    return pl.CostEstimate(flops=bytes_, bytes_accessed=bytes_, transcendentals=0)


def small():
    return pltpu.CompilerParams(vmem_limit_bytes=GRANT)


def vmem():
    return pl.BlockSpec(memory_space=pltpu.VMEM)


def anywhere():
    return pl.BlockSpec(memory_space=pltpu.HBM)


def as_row(column):
    return column.T[0:1, :]


def as_column(row, side):
    lanes = jnp.broadcast_to(row, (128, side)).T
    return jnp.concatenate([lanes] * (side // 128), axis=1)


def code(x, by_column):
    side = x.shape[0]
    size = jnp.abs(x)
    if by_column:
        top = jnp.max(size, axis=0, keepdims=True)
        row = jnp.maximum((top * 1.01).astype(jnp.bfloat16).astype(F32), LEAST)
        scale = row
    else:
        top = jnp.broadcast_to(jnp.max(size, axis=1, keepdims=True), (side, 128))
        lanes = jnp.maximum((top * 1.01).astype(jnp.bfloat16).astype(F32), LEAST)
        row = as_row(lanes)
        scale = jnp.concatenate([lanes] * (side // 128), axis=1)
    level = jnp.round(size * (LEVELS / scale))
    power = jnp.floor(level * (1.0 / 1024.0))
    number = (level + (1024.0 - 1024.0 * power)) * jnp.exp2(power - 24.0)
    return jnp.where(x < 0, -number, number), row


def decode(number, row, by_column):
    side = number.shape[0]
    size = jnp.abs(number)
    power = jnp.floor(jnp.log2(size * (1.0 + 2.0**-12)) + 14.0)
    level = 1024.0 * (power + size * jnp.exp2(14.0 - power) - 1.0)
    unit = row * (1.0 / LEVELS)
    unit = unit if by_column else as_column(unit, side)
    return jnp.where(number < 0, -level, level) * unit


def write_message(out, blocks, norm, columns, side):
    k = len(blocks)
    rows = []
    for j in range(k):
        number, row = code(blocks[j], columns[j])
        out[j * side : (j + 1) * side, :] = number
        rows.append(row * ROW_SCALE)
    if norm is not None:
        norm = norm * NORM_SCALE
        high = norm.astype(jnp.bfloat16).astype(F32)
        rows += [high, norm - high]
    for j in range(PAD):
        out[k * side + j : k * side + j + 1, :] = rows[min(j, len(rows) - 1)]


def read_message(got, columns, with_norm, side):
    k = len(columns)
    row = lambda j: got[k * side + j : k * side + j + 1, :]
    blocks = [
        decode(got[j * side : (j + 1) * side, :], row(j) * (1.0 / ROW_SCALE), columns[j])
        for j in range(k)
    ]
    norm = (row(k) + row(k + 1)) * (1.0 / NORM_SCALE) if with_norm else None
    return blocks, norm


def fetch(grad_refs, held, sem, columns, slot, side):
    start = pl.multiple_of((lax.axis_index("replica") ^ slot) * side, side)
    moves = []
    for j, ref in enumerate(grad_refs):
        part = ref.at[0, :, pl.ds(start, side)] if columns[j] else ref.at[0, pl.ds(start, side), :]
        moves.append(pltpu.make_async_copy(part, held.at[j], sem.at[j]))
    for move in moves:
        move.start()
    return moves


def fetch_norm(norm_ref, held, sem, slot, side):
    start = pl.multiple_of((lax.axis_index("replica") ^ slot) * side, side)
    move = pltpu.make_async_copy(norm_ref.at[:, pl.ds(start, side)], held, sem)
    move.start()
    return move


def send_block(grads, columns, norm, got, side, slot):
    k = len(grads)
    rows = k * side + PAD

    def body(*refs):
        refs = list(refs)
        grad_refs = [refs.pop(0) for _ in range(k)]
        norm_ref = refs.pop(0) if norm is not None else None
        got_ref = refs.pop(0) if got is not None else None
        out, held, sem = refs[:3]
        moves = fetch(grad_refs, held, sem, columns, slot, side)
        if norm is not None:
            moves.append(fetch_norm(norm_ref, refs[3], sem.at[k], slot, side))
        more, more_norm = [None] * k, None
        if got is not None:
            more, more_norm = read_message(got_ref, columns, norm is not None, side)
        for move in moves:
            move.wait()
        row = None
        if norm is not None:
            row = refs[3][...] if more_norm is None else refs[3][...] + more_norm
        blocks = [held[j] if more[j] is None else held[j] + more[j] for j in range(k)]
        write_message(out, blocks, row, columns, side)

    specs, args = [anywhere()] * k, list(grads)
    if norm is not None:
        specs.append(anywhere())
        args.append(norm)
    if got is not None:
        specs.append(vmem())
        args.append(got)
    return pl.pallas_call(
        body,
        out_shape=jax.ShapeDtypeStruct((rows, side), F32),
        in_specs=specs,
        out_specs=vmem(),
        scratch_shapes=[
            pltpu.VMEM((k, side, side), F32),
            pltpu.SemaphoreType.DMA((k + 1,)),
            pltpu.VMEM((1, side), F32),
        ],
        cost_estimate=cost(k * side * side * 16),
        compiler_params=small(),
    )(*args)


def slice_sums(square, by_column):
    if by_column:
        return jnp.sum(square, axis=0, keepdims=True)
    side = square.shape[0]
    lanes = square[:, :128]
    for start in range(128, side, 128):
        lanes = lanes + square[:, start : start + 128]
    return jnp.sum(lanes.T, axis=0, keepdims=True)


def means(grads, columns, norm, weights, gots, side, rate):
    k = len(grads)

    def body(*refs):
        refs = list(refs)
        grad_refs = [refs.pop(0) for _ in range(k)]
        norm_ref = refs.pop(0) if norm is not None else None
        weight_refs = [refs.pop(0) for _ in range(k)]
        got_refs = [refs.pop(0) for _ in gots]
        mean_ref, sum_ref, held, sem, held_weights, held_norm = refs
        moves = fetch(grad_refs, held, sem, columns, 0, side)
        for j in range(k):
            moves.append(pltpu.make_async_copy(weight_refs[j], held_weights.at[j], sem.at[k + j]))
            moves[-1].start()
        if norm is not None:
            moves.append(fetch_norm(norm_ref, held_norm, sem.at[2 * k], 0, side))
        totals, row = [None] * k, None
        for got_ref in got_refs:
            blocks, more = read_message(got_ref, columns, norm is not None, side)
            totals = [b if t is None else t + b for t, b in zip(totals, blocks)]
            row = more if row is None else row + more
        for move in moves:
            move.wait()
        for j in range(k):
            mean = (held[j] + totals[j]) * rate
            mean_ref[j * side : (j + 1) * side, :] = mean
            weight = held_weights[j]
            sum_ref[2 * j : 2 * j + 1, :] = slice_sums(weight * weight, columns[j])
            sum_ref[2 * j + 1 : 2 * j + 2, :] = slice_sums(mean * mean, columns[j])
        if norm is not None:
            mean_ref[k * side :, :] = jnp.broadcast_to((held_norm[...] + row) * rate, (PAD, side))

    specs, args = [anywhere()] * k, list(grads)
    if norm is not None:
        specs.append(anywhere())
        args.append(norm)
    args += [*weights, *gots]
    specs += [anywhere()] * k + [vmem()] * len(gots)
    rows = k * side + (PAD if norm is not None else 0)
    return pl.pallas_call(
        body,
        out_shape=[
            jax.ShapeDtypeStruct((rows, side), F32),
            jax.ShapeDtypeStruct((2 * k, side), F32),
        ],
        in_specs=specs,
        out_specs=[vmem()] * 2,
        scratch_shapes=[
            pltpu.VMEM((k, side, side), F32),
            pltpu.SemaphoreType.DMA((2 * k + 1,)),
            pltpu.VMEM((k, side, side), F32),
            pltpu.VMEM((1, side), F32),
        ],
        cost_estimate=cost(k * side * side * 24),
        compiler_params=small(),
    )(*args)


def update(mean, sums, weights, moments, columns, norm, side):
    k = len(weights)

    def body(*refs):
        refs = list(refs)
        mean_ref = refs.pop(0)
        sum_refs = [refs.pop(0) for _ in sums]
        weight_refs = [refs.pop(0) for _ in range(k)]
        moment_refs = [refs.pop(0) for _ in range(k)]
        norm_refs = [refs.pop(0) for _ in range(2)] if norm is not None else []
        held, sem = refs[-2:]
        moves = [pltpu.make_async_copy(r, held.at[i], sem.at[i]) for i, r in enumerate(norm_refs)]
        for move in moves:
            move.start()
        send_ref = refs.pop(0)
        new_refs = [refs.pop(0) for _ in range(k)]
        state_refs = [refs.pop(0) for _ in range(k)]
        total = sum_refs[0][...]
        for s in sum_refs[1:]:
            total = total + s[...]
        for j in range(k):
            part = slice(j * side, (j + 1) * side)
            ratio = jnp.sqrt(total[2 * j : 2 * j + 1, :]) * lax.rsqrt(
                total[2 * j + 1 : 2 * j + 2, :] + 1e-06
            )
            full = ratio if columns[j] else as_column(ratio, side)
            state = hold_rate * moment_refs[j][...] + mean_ref[part, :] * full
            new = weight_refs[j][...] - learn_rate * state
            state_refs[j][...] = state
            new_refs[j][...] = new
            send_ref[part, :] = new.astype(jnp.bfloat16)
        if norm is not None:
            new_ref, state_ref = refs.pop(0), refs.pop(0)
            for move in moves:
                move.wait()
            row = mean_ref[k * side : k * side + 1, :]
            state = hold_rate * held[1] + row
            new = held[0] - learn_rate * state
            state_ref[...] = state
            new_ref[...] = new
            send_ref[k * side :, :] = jnp.broadcast_to(new, (PAD, side)).astype(jnp.bfloat16)

    args = [mean, *sums, *weights, *moments]
    square = jax.ShapeDtypeStruct((side, side), F32)
    outs = [jax.ShapeDtypeStruct(mean.shape, jnp.bfloat16)] + [square] * (2 * k)
    specs = [vmem() for _ in args]
    if norm is not None:
        args += list(norm)
        specs += [anywhere()] * 2
        outs += [jax.ShapeDtypeStruct((1, side), F32)] * 2
    return pl.pallas_call(
        body,
        out_shape=outs,
        in_specs=specs,
        out_specs=[vmem() for _ in outs],
        scratch_shapes=[pltpu.VMEM((2, 1, side), F32), pltpu.SemaphoreType.DMA((2,))],
        cost_estimate=cost(k * side * side * 22),
        compiler_params=small(),
    )(*args)


def assemble(blocks, columns, with_norm, side):
    k, n = len(columns), len(blocks)

    def body(*refs):
        ins, outs, sem = refs[:n], refs[n:-1], refs[-1]
        starts = [
            pl.multiple_of((lax.axis_index("replica") ^ slot) * side, side) for slot in range(n)
        ]
        moves = []
        for slot in range(n):
            for j in range(k):
                part = ins[slot].at[j * side : (j + 1) * side, :]
                if columns[j]:
                    to = outs[j].at[:, pl.ds(starts[slot], side)]
                else:
                    to = outs[j].at[pl.ds(starts[slot], side), :]
                moves.append(pltpu.make_async_copy(part, to, sem.at[slot * k + j]))
        for move in moves:
            move.start()
        if with_norm:
            for slot in range(n):
                row = ins[slot][k * side : k * side + 1, :]
                outs[k][0:1, pl.ds(starts[slot], side)] = row
        for move in moves:
            move.wait()

    outs, specs = [], []
    for c in columns:
        shape = (side, n * side) if c else (n * side, side)
        outs.append(jax.ShapeDtypeStruct(shape, jnp.bfloat16))
        specs.append(anywhere())
    if with_norm:
        outs.append(jax.ShapeDtypeStruct((1, n * side), jnp.bfloat16))
        specs.append(vmem())
    return pl.pallas_call(
        body,
        out_shape=outs,
        in_specs=[vmem()] * n,
        out_specs=specs,
        scratch_shapes=[pltpu.SemaphoreType.DMA((n * k,))],
        cost_estimate=cost(n * k * side * side * 4),
        compiler_params=small(),
    )(*blocks)


def four(
    grad_query,
    grad_key,
    grad_value,
    grad_mixed,
    grad_norm,
    weight_query,
    weight_key,
    weight_value,
    weight_mixed,
    weight_norm,
    moment_query,
    moment_key,
    moment_value,
    moment_mixed,
    moment_norm,
):
    n, m = lax.axis_size("replica"), lax.axis_size("model")
    side = weight_query.shape[0]
    rate = n ** (-0.5)

    def swap(x, bit, axis="replica"):
        return lax.ppermute(x, axis, [(i, i ^ bit) for i in range(lax.axis_size(axis))])

    def carry(x, bit):
        return swap(x.astype(WIRE), bit).astype(F32)

    far_off = lambda xs: tuple(pltpu.with_memory_space_constraint(x, pltpu.HBM) for x in xs)
    grads = far_off((grad_query, grad_key, grad_value, grad_mixed))
    weights = (weight_query, weight_key, weight_value, weight_mixed)
    moments = (moment_query, moment_key, moment_value, moment_mixed)
    columns = (False, False, False, True)
    norm_values = far_off((weight_norm.reshape(1, side), moment_norm.reshape(1, side)))
    copies, news, states = {}, {}, {}
    for tag, group, has_norm in (("a", (0, 1), True), ("b", (2, 3), False)):
        pick = lambda xs: [xs[j] for j in group]
        cols, own_grads = pick(columns), pick(grads)
        norm = far_off((grad_norm,))[0] if has_norm else None

        def block(slot, got):
            return send_block(own_grads, cols, norm, got, side, slot)

        if tag == "a":
            far = carry(block(3, None), 1)
            near = carry(block(1, None), 1)
            gots = [near, carry(block(2, far), 2)]
        else:
            gots = [carry(block(slot, None), slot) for slot in (3, 2, 1)]
        mean, sums = means(own_grads, cols, norm, far_off(pick(weights)), gots, side, rate)
        parts = [sums] + [swap(sums, bit, "model") for bit in range(1, m)]
        out = update(
            mean, parts, pick(weights), pick(moments), cols,
            norm_values if has_norm else None, side,
        )
        own = out[0]
        two = swap(own, 2)
        one = swap(own, 1)
        three = swap(two, 1) if tag == "a" else swap(own, 3)
        whole = assemble([own, one, two, three], cols, has_norm, side)
        k = len(group)
        for i, j in enumerate(group):
            copies[j], news[j], states[j] = whole[i], out[1 + i], out[1 + k + i]
        if has_norm:
            copies[4] = whole[k].reshape(-1)
            news[4], states[4] = out[1 + 2 * k].reshape(-1), out[2 + 2 * k].reshape(-1)
    return tuple(d[j] for d in (copies, news, states) for j in range(5))


def local(*args):
    n, m = lax.axis_size("replica"), lax.axis_size("model")
    rows, _ = args[5].shape
    square = all(a.shape == (rows, rows) for a in args[5:9]) and rows % 128 == 0
    if n == 4 and m & (m - 1) == 0 and square and args[9].shape == (rows,):
        return four(*args)
    return general(*args)


def solution(mesh):
    lead, wide = ("job", "replica"), ("job", "model")
    grads = (P(lead, None, "model"),) * 3 + (P(lead, "model", None), P(lead, None))
    shards = (P(lead, "model"),) * 3 + (P(wide, "replica"), P(lead))
    copies = (P("job", "model"),) * 3 + (P(wide, None), P("job"))
    return jax.shard_map(
        local,
        mesh=mesh,
        in_specs=grads + shards + shards,
        out_specs=copies + shards + shards,
        check_vma=False,
    )
```
